128 devices in a mesh: gx: 8 (over x, core), gy: 16 (over y, z).
Axes of the slice: x: 4, y: 4, z: 4, core: 2. Of those that a mesh axis runs over, the one named last changes fastest.
Arguments:
- tokens: bfloat16 [512, 8192], P('gy', 'gx'), may hold values from -6 to 6
- up_old: bfloat16 [32768, 8192], P(('gx', 'gy')), may hold values from -0.0625 to 0.0625
- down_old: bfloat16 [32768, 8192], P(('gx', 'gy')), may hold values from -0.0625 to 0.0625
- old_slot: int32 [256], replicated, may hold values from 0 to 255, as said below
- new_owner: int32 [256], replicated, may hold values from 0 to 127, as said below
- hot_rank: int32 [256], replicated, may hold values from 0 to 1, as said below
- route: int32 [512], replicated, may hold values from 0 to 511, each once
Outputs:
- up_new: bfloat16 [32768, 8192], P(('gx', 'gy'))
- down_new: bfloat16 [32768, 8192], P(('gx', 'gy'))
- mixed: bfloat16 [512, 8192], P('gy', 'gx')
The draws below stay inside these ranges and needn't reach their ends.
Inputs may be any that keep to these rules, and one draw needn't show every extreme that they name: `old_slot`: each slot number appears exactly once. `new_owner`: each device index is the new owner of exactly 2 blocks. `hot_rank`: the blocks of one new owner have distinct ranks.
All inputs are finite; a program needn't handle non-finite values.
Results may differ from the reference program's by a relative error of at most 0.0049.
Values may be sent and summed in bfloat16 or wider, within the bound.
A program may use at most 128 MiB of HBM per device.

```python
import jax
import jax.numpy as jnp
from jax import lax

D = 8192
BLOCK = 128
BLK_DEV = 2
FF = 32768
NBLK = 256
TOKENS = 512


def draw_old_slot(key, part):
    return jax.random.permutation(jax.random.fold_in(key, 11), NBLK).astype(jnp.int32)


def shared_order(key):
    return jax.random.permutation(jax.random.fold_in(key, 23), NBLK).astype(jnp.int32)


def draw_new_owner(key, part):
    return (shared_order(key) // BLK_DEV).astype(jnp.int32)


def draw_hot_rank(key, part):
    return (shared_order(key) % BLK_DEV).astype(jnp.int32)


def levels(stream_key, shape, cuts, least, high):
    factor_of, own = 1.0, jax.random.fold_in(stream_key, 6)
    for axis_at, blocks in cuts:
        draws = jnp.exp(jax.random.uniform(jax.random.fold_in(own, axis_at), (blocks,), jnp.float32, least / len(cuts), high / len(cuts)))
        factor_of = factor_of * jnp.repeat(draws, shape[axis_at] // blocks).reshape([-1 if axis == axis_at else 1 for axis in range(len(shape))])
    return factor_of


def scatter_about(rng, shape, width, most, cuts=(), held_as=jnp.bfloat16):
    factor_of = levels(rng, shape, cuts, -0.22, 0.18) if cuts else 1.0
    values = jax.random.normal(rng, shape, jnp.float32) * width * factor_of
    return jnp.minimum(jnp.maximum(values, -most), most).astype(held_as)


def setup_inputs(seed: int = 0) -> dict:
    key_list = jax.random.split(jax.random.key(seed), 8)
    return {
        "tokens": scatter_about(key_list[0], (TOKENS, D), 1.0, 6.0, ((0, 16), (1, 8))),
        "up_old": scatter_about(key_list[1], (FF, D), D ** -0.5, 0.0625, ((0, 128),)),
        "down_old": scatter_about(key_list[2], (FF, D), (FF // 4) ** -0.5, 0.0625, ((0, 128),)),
        "old_slot": draw_old_slot(jax.random.fold_in(key_list[7], 71), 0),
        "new_owner": draw_new_owner(jax.random.fold_in(key_list[7], 71), 0),
        "hot_rank": draw_hot_rank(jax.random.fold_in(key_list[7], 71), 0),
        "route": jax.random.permutation(key_list[6], TOKENS).astype(jnp.int32),
    }


def reference(tokens, up_old, down_old, old_slot, new_owner, hot_rank, route):
    new_slot = (new_owner * BLK_DEV + hot_rank).astype(jnp.int32)
    source = jnp.zeros((NBLK,), jnp.int32).at[new_slot].set(old_slot.astype(jnp.int32))
    up_new = up_old.reshape(NBLK, BLOCK, D)[source].reshape(FF, D)
    down_new = down_old.reshape(NBLK, BLOCK, D)[source].reshape(FF, D)
    ordered = tokens[route.astype(jnp.int32)]
    pre = lax.dot_general(ordered, up_old, (((1,), (1,)), ((), ())), preferred_element_type=jnp.float32)
    hidden = jax.nn.gelu(pre, approximate=False).astype(jnp.bfloat16)
    mixed = jnp.dot(hidden, down_old, preferred_element_type=jnp.float32).astype(jnp.bfloat16)
    return up_new, down_new, mixed
```

```python
import jax
import jax.numpy as jnp
from jax import lax
from jax.experimental import pallas as pl
from jax.experimental.pallas import tpu as pltpu
from jax.sharding import PartitionSpec as P

MESH = pl.DeviceIdType.MESH
BF = jnp.bfloat16
F32 = jnp.float32

PLANE = ((1, 0), (0, 1), (3, 0), (0, 3), (1, 3), (3, 1), (2, 0), (0, 2), (1, 1), (3, 3), (2, 1), (2, 3), (1, 2), (3, 2), (2, 2))
LINE = ((0, 1), (1, 0), (3, 0), (1, 1), (3, 1), (2, 0), (2, 1))

ERFC_P = (2.326819970068386e-2, -1.387039388740657e-1, 3.687424674597105e-1, -5.824733027278666e-1, 6.210004621745983e-1,
          -4.944515323274145e-1, 3.404879937665872e-1, -2.741127028184656e-1, 5.638259427386472e-1)
ERFC_R = (-1.047766399936249e1, 1.297719955372516e1, -7.495518717768503e0, 2.921019019210786e0, -1.015265279202700e0,
          4.218463358204948e-1, -2.820767439740514e-1, 5.641895067754075e-1)
ERF_T = (7.853861353153693e-5, -8.010193625184903e-4, 5.188327685732524e-3, -2.685381193529856e-2, 1.128358514861418e-1,
         -3.761262582423300e-1, 1.128379165726710e0)


def poly(y, coefficients):
    total = jnp.full_like(y, coefficients[0])
    for c in coefficients[1:]:
        total = total * y + c
    return total


def erfc(v):
    size = jnp.maximum(jnp.abs(v), 0.5)
    q = 1.0 / size
    y = q * q
    tail = jnp.exp(-v * v) * q * jnp.where(size < 2.0, poly(y, ERFC_P), poly(y, ERFC_R))
    far = jnp.where(v < 0.0, 2.0 - tail, tail)
    near = 1.0 - v * poly(v * v, ERF_T)
    return jnp.where(jnp.abs(v) > 1.0, far, near)


def gelu(v):
    return 0.5 * v * erfc(v * -0.7071067811865476)


SEMS = ("s1u", "s1d", "s2u", "s2d", "s3u", "s3d", "s4u", "s4d", "agy", "agz", "agx", "agc", "agd", "rc", "ry", "rz", "rx", "wu", "wd", "tok")


def kernel(source, route, tokens, up, down, up2, down2, up_new, down_new, mixed, s1u, s1d, s3u, s3d,
           s2u, s2d, pu, pd, t, upv, downv, pre, hid, acc, sc, rc, ry, sz, rz, sx, rx, send, recv):
    gx, gy = lax.axis_index("gx"), lax.axis_index("gy")
    x, c = gx // 2, lax.rem(gx, 2)
    y, z = gy // 4, lax.rem(gy, 4)
    plane = [lax.rem(y + dy, 4) * 4 + lax.rem(z + dz, 4) for dy, dz in PLANE]
    line = [lax.rem(x + dx, 4) * 2 + lax.rem(c + dc, 2) for dx, dc in LINE]
    xs = [lax.rem(x + d, 4) for d in (1, 2, 3)]
    ys = [lax.rem(y + d, 4) for d in (1, 2, 3)]
    zs = [lax.rem(z + d, 4) for d in (1, 2, 3)]
    other = 1 - c
    at = {name: i for i, name in enumerate(SEMS)}

    def push(name, src, dst, where):
        pltpu.make_async_remote_copy(
            src_ref=src, dst_ref=dst, send_sem=send.at[at[name]], recv_sem=recv.at[at[name]], device_id=where, device_id_type=MESH
        ).start()

    def keep(name, src, dst):
        pltpu.make_async_copy(src, dst, recv.at[at[name]]).start()

    def got(name, ref):
        pltpu.make_async_copy(ref, ref, recv.at[at[name]]).wait()

    def sent(name, ref):
        pltpu.make_async_copy(ref, ref, send.at[at[name]]).wait()

    def cols(g):
        return pl.ds(pl.multiple_of(g * 1024, 1024), 1024)

    barrier = pltpu.get_barrier_semaphore()
    for p in plane:
        pl.semaphore_signal(barrier, inc=1, device_id={"gy": p}, device_id_type=MESH)
    for p in line:
        pl.semaphore_signal(barrier, inc=1, device_id={"gx": p}, device_id_type=MESH)
    pl.semaphore_wait(barrier, len(PLANE) + len(LINE))

    keep("tok", tokens, t.at[y, z, :, cols(gx)])
    for p in ys:
        push("agy", tokens, t.at[y, z, :, cols(gx)], {"gy": p * 4 + z})
    for p in line:
        push("s1d", down.at[:, :, :, cols(p)], s1d.at[gx], {"gx": p})
    keep("s1d", down.at[:, :, :, cols(gx)], s1d.at[gx])
    keep("wu", up2, upv)
    keep("wd", down2, downv)
    got("tok", tokens)
    got("agy", t.at[0, 0:3, :, pl.ds(0, 1024)])
    for p in zs:
        push("agz", t.at[:, z, :, cols(gx)], t.at[:, z, :, cols(gx)], {"gy": y * 4 + p})
    for p in plane:
        push("s1u", up.at[:, p], s1u.at[pl.ds(gy * 2, 2)], {"gy": p})
    keep("s1u", up.at[:, gy], s1u.at[pl.ds(gy * 2, 2)])
    got("agz", t.at[:, 0:3, :, pl.ds(0, 1024)])
    for p in xs:
        push("agx", t.at[:, :, :, cols(gx)], t.at[:, :, :, cols(gx)], {"gx": p * 2 + c})
    push("agc", t.at[:, :, :, cols(gx)], t.at[:, :, :, cols(gx)], {"gx": x * 2 + other})
    got("s1d", s1d)
    for p in plane:
        push("s2d", s1d.at[:, :, p], s2d.at[:, gy], {"gy": p})
    keep("s2d", s1d.at[:, :, gy], s2d.at[:, gy])
    got("s1u", s1u)
    for p in line:
        push("s2u", s1u.at[:, :, cols(p)], s2u.at[pl.ds(gx * 32, 32)], {"gx": p})
    keep("s2u", s1u.at[:, :, cols(gx)], s2u.at[pl.ds(gx * 32, 32)])
    got("agx", t.at[:, :, :, pl.ds(0, 3072)])
    for p in xs:
        push("agd", t.at[:, :, :, cols(p * 2 + c)], t.at[:, :, :, cols(p * 2 + c)], {"gx": x * 2 + other})
    got("agc", t.at[:, :, :, pl.ds(0, 1024)])
    got("agd", t.at[:, :, :, pl.ds(0, 3072)])

    got("wu", upv)
    pre[...] = jnp.zeros_like(pre)

    def first(k, carry):
        w = upv[:, pl.ds(pl.multiple_of(k * 1024, 1024), 1024)]

        def rows(m, inner):
            a = t[m, :, :, pl.ds(pl.multiple_of(k * 1024, 1024), 1024)].reshape(128, 1024)
            at_rows = pl.ds(pl.multiple_of(m * 128, 128), 128)
            pre[at_rows, :] += lax.dot_general(a, w, (((1,), (1,)), ((), ())), preferred_element_type=F32)
            return inner

        return lax.fori_loop(0, 4, rows, carry)

    lax.fori_loop(0, 8, first, 0)

    def act(m, carry):
        at_rows = pl.ds(pl.multiple_of(m * 64, 64), 64)
        hid[at_rows, :] = gelu(pre[at_rows, :]).astype(BF)
        return carry

    lax.fori_loop(0, 8, act, 0)

    def order(m, carry):
        at_rows = pl.ds(pl.multiple_of(m * 128, 128), 128)
        pick = jnp.where(route[at_rows, :] == lax.broadcasted_iota(jnp.int32, (128, 512), 1), 1.0, 0.0).astype(BF)
        pre[at_rows, :] = jnp.dot(pick, hid[...], preferred_element_type=F32)
        return carry

    lax.fori_loop(0, 4, order, 0)
    hid[...] = pre[...].astype(BF)
    got("wd", downv)

    for q in range(4):
        def theirs(m, carry):
            at_rows = pl.ds(pl.multiple_of(m * 128, 128), 128)
            sc[q, at_rows, :] = jnp.dot(hid[at_rows, :], downv[:, cols(q * 2 + other)], preferred_element_type=F32).astype(BF)
            return carry

        lax.fori_loop(0, 4, theirs, 0)
        push("rc", sc.at[q], rc.at[q], {"gx": x * 2 + other})

    def permute_down(n, carry):
        s = source[n]
        pd[n // 32, lax.rem(n // 2, 16), lax.rem(n, 2)] = s2d[s // 32, lax.rem(s // 2, 16), lax.rem(s, 2)]
        return carry

    got("s2d", s2d)
    lax.fori_loop(0, 256, permute_down, 0)
    for p in plane:
        push("s3d", pd.at[:, p], s3d.at[:, :, gy], {"gy": p})
    keep("s3d", pd.at[:, gy], s3d.at[:, :, gy])

    def mine(m, carry):
        at_rows = pl.ds(pl.multiple_of(lax.rem(m, 4) * 128, 128), 128)
        acc[m // 4, at_rows, :] = jnp.dot(hid[at_rows, :], downv[:, cols((m // 4) * 2 + c)], preferred_element_type=F32)
        return carry

    lax.fori_loop(0, 16, mine, 0)
    sent("rc", sc)
    got("rc", rc)

    def both(m, carry):
        q, at_rows = m // 8, pl.ds(pl.multiple_of(lax.rem(m, 8) * 64, 64), 64)
        total = acc[q, at_rows, :] + rc[q, at_rows, :].astype(F32)
        acc[q, at_rows, :] = total
        sc[q, at_rows, :] = total.astype(BF)
        return carry

    lax.fori_loop(0, 32, both, 0)
    for i, p in enumerate(ys):
        push("ry", sc.at[:, pl.ds(pl.multiple_of(p * 128, 128), 128), :], ry.at[i], {"gy": p * 4 + z})

    def permute_up(n, carry):
        pu[n] = s2u[source[n]]
        return carry

    got("s2u", s2u)
    lax.fori_loop(0, 256, permute_up, 0)
    for p in line:
        push("s3u", pu.at[pl.ds(p * 32, 32)], s3u.at[:, :, cols(gx)], {"gx": p})
    keep("s3u", pu.at[pl.ds(gx * 32, 32)], s3u.at[:, :, cols(gx)])

    got("s3d", s3d)
    for p in line:
        push("s4d", s3d.at[p], down_new.at[:, :, :, cols(gx)], {"gx": p})
    keep("s4d", s3d.at[gx], down_new.at[:, :, :, cols(gx)])

    got("ry", ry)

    def over_y(m, carry):
        q, r = m // 2, pl.multiple_of(lax.rem(m, 2) * 64, 64)
        at_rows = pl.ds(pl.multiple_of(y * 128 + r, 64), 64)
        total = acc[q, at_rows, :]
        for i in range(3):
            total = total + ry[i, q, pl.ds(r, 64), :].astype(F32)
        acc[q, at_rows, :] = total
        sz[q, pl.ds(r, 64), :] = total.astype(BF)
        return carry

    lax.fori_loop(0, 8, over_y, 0)
    for i, p in enumerate(zs):
        push("rz", sz.at[:, pl.ds(pl.multiple_of(p * 32, 32), 32), :], rz.at[i], {"gy": y * 4 + p})

    got("s3u", s3u)
    for p in plane:
        push("s4u", s3u.at[pl.ds(p * 2, 2)], up_new.at[:, gy], {"gy": p})
    keep("s4u", s3u.at[pl.ds(gy * 2, 2)], up_new.at[:, gy])

    got("rz", rz)
    here = pl.ds(pl.multiple_of(y * 128 + z * 32, 32), 32)

    def over_z(q, carry):
        total = acc[q, here, :]
        for i in range(3):
            total = total + rz[i, q].astype(F32)
        acc[q, here, :] = total
        sx[q] = total.astype(BF)
        return carry

    lax.fori_loop(0, 4, over_z, 0)
    for i, p in enumerate(xs):
        push("rx", sx.at[p], rx.at[i], {"gx": p * 2 + c})
    got("rx", rx)
    total = acc[x, here, :]
    for i in range(3):
        total = total + rx[i].astype(F32)
    mixed[...] = total.astype(BF)

    got("s4d", s1d)
    got("s4u", s1u)
    for name in ("s1u", "s2d", "s3d", "s4u"):
        sent(name, s1u.at[pl.ds(0, 30)])
    for name in ("s1d", "s2u", "s3u", "s4d"):
        sent(name, s1d.at[pl.ds(0, 7)])
    sent("agy", t.at[0, 0:3, :, pl.ds(0, 1024)])
    sent("agz", t.at[:, 0:3, :, pl.ds(0, 1024)])
    sent("agx", t.at[:, :, :, pl.ds(0, 3072)])
    sent("agc", t.at[:, :, :, pl.ds(0, 1024)])
    sent("agd", t.at[:, :, :, pl.ds(0, 3072)])
    sent("ry", ry)
    sent("rz", rz)
    sent("rx", rx)


def shards(tokens, up_old, down_old, old_slot, new_owner, hot_rank, route):
    new_slot = new_owner * 2 + hot_rank
    slots = lax.broadcasted_iota(jnp.int32, (256, 256), 0)
    source = jnp.sum(jnp.where(slots == new_slot[None, :], old_slot[None, :], 0), axis=1)
    up4, down4 = up_old.reshape(2, 16, 8, 8192), down_old.reshape(2, 16, 8, 8192)
    any_, vmem = pl.BlockSpec(memory_space=pl.ANY), pl.BlockSpec(memory_space=pltpu.VMEM)
    block = jax.ShapeDtypeStruct((2, 16, 8, 8192), BF)
    outs = pl.pallas_call(
        kernel,
        out_shape=(
            block, block, jax.ShapeDtypeStruct((32, 1024), BF),
            jax.ShapeDtypeStruct((32, 8, 8192), BF), jax.ShapeDtypeStruct((8, 2, 16, 8, 1024), BF),
            jax.ShapeDtypeStruct((32, 8, 8192), BF), jax.ShapeDtypeStruct((8, 2, 16, 8, 1024), BF),
        ),
        in_specs=[pl.BlockSpec(memory_space=pltpu.SMEM), vmem, any_, any_, any_, any_, any_],
        out_specs=(any_, any_, vmem, any_, any_, any_, any_),
        scratch_shapes=[
            pltpu.VMEM((256, 8, 1024), BF), pltpu.VMEM((8, 16, 2, 8, 1024), BF),
            pltpu.VMEM((256, 8, 1024), BF), pltpu.VMEM((8, 16, 2, 8, 1024), BF),
            pltpu.VMEM((4, 4, 32, 8192), BF), pltpu.VMEM((256, 8192), BF), pltpu.VMEM((256, 8192), BF),
            pltpu.VMEM((512, 256), F32), pltpu.VMEM((512, 256), BF),
            pltpu.VMEM((4, 512, 1024), F32), pltpu.VMEM((4, 512, 1024), BF), pltpu.VMEM((4, 512, 1024), BF),
            pltpu.VMEM((3, 4, 128, 1024), BF), pltpu.VMEM((4, 128, 1024), BF), pltpu.VMEM((3, 4, 32, 1024), BF),
            pltpu.VMEM((4, 32, 1024), BF), pltpu.VMEM((3, 32, 1024), BF),
            pltpu.SemaphoreType.DMA((len(SEMS),)), pltpu.SemaphoreType.DMA((len(SEMS),)),
        ],
        compiler_params=pltpu.CompilerParams(collective_id=0, has_side_effects=True, vmem_limit_bytes=67043328),
    )(source, route.reshape(512, 1), tokens, up4, down4, up_old, down_old)
    return outs[0].reshape(256, 8192), outs[1].reshape(256, 8192), outs[2]


def solution(mesh):
    in_specs = (P("gy", "gx"), P(("gx", "gy"), None), P(("gx", "gy"), None), P(), P(), P(), P())
    out_specs = (P(("gx", "gy"), None), P(("gx", "gy"), None), P("gy", "gx"))
    return jax.shard_map(shards, mesh=mesh, in_specs=in_specs, out_specs=out_specs, check_vma=False)
```

```python
import jax
import jax.numpy as jnp
from jax import lax
from jax.experimental import pallas as pl
from jax.experimental.pallas import tpu as pltpu
from jax.sharding import PartitionSpec as P

MESH = pl.DeviceIdType.MESH
BF = jnp.bfloat16
F32 = jnp.float32

PLANE = ((1, 0), (0, 1), (3, 0), (0, 3), (1, 3), (3, 1), (2, 0), (0, 2), (1, 1), (3, 3), (2, 1), (2, 3), (1, 2), (3, 2), (2, 2))
LINE = ((0, 1), (1, 0), (3, 0), (1, 1), (3, 1), (2, 0), (2, 1))

ERFC_P = (2.326819970068386e-2, -1.387039388740657e-1, 3.687424674597105e-1, -5.824733027278666e-1, 6.210004621745983e-1,
          -4.944515323274145e-1, 3.404879937665872e-1, -2.741127028184656e-1, 5.638259427386472e-1)
ERFC_R = (-1.047766399936249e1, 1.297719955372516e1, -7.495518717768503e0, 2.921019019210786e0, -1.015265279202700e0,
          4.218463358204948e-1, -2.820767439740514e-1, 5.641895067754075e-1)
ERF_T = (7.853861353153693e-5, -8.010193625184903e-4, 5.188327685732524e-3, -2.685381193529856e-2, 1.128358514861418e-1,
         -3.761262582423300e-1, 1.128379165726710e0)


def poly(y, coefficients):
    total = jnp.full_like(y, coefficients[0])
    for c in coefficients[1:]:
        total = total * y + c
    return total


def erfc(v):
    size = jnp.maximum(jnp.abs(v), 0.5)
    q = 1.0 / size
    y = q * q
    tail = jnp.exp(-v * v) * q * jnp.where(size < 2.0, poly(y, ERFC_P), poly(y, ERFC_R))
    far = jnp.where(v < 0.0, 2.0 - tail, tail)
    near = 1.0 - v * poly(v * v, ERF_T)
    return jnp.where(jnp.abs(v) > 1.0, far, near)


def gelu(v):
    return 0.5 * v * erfc(v * -0.7071067811865476)


NAMES = ("s1u", "s1d", "s2u", "s2d", "s3u", "s3d", "s4u", "s4d", "pc", "px")
SINGLE = ("tok", "agy", "agz", "hx", "hc", "hd", "ry", "rz")
AT = {(name, h): 2 * i + h for i, name in enumerate(NAMES) for h in (0, 1)}
AT.update({(name, 0): 2 * len(NAMES) + i for i, name in enumerate(SINGLE)})


def kernel(source, route, tokens, up, down, up_new, down_new, mixed, s1u, s1d, s3u, s3d,
           s2u, s2d, pu, pd, t, to, pr, pc, px, hid, hb, acc, sc, ry, sz, rz, send, recv):
    gx, gy = lax.axis_index("gx"), lax.axis_index("gy")
    x, c = gx // 2, lax.rem(gx, 2)
    y, z = gy // 4, lax.rem(gy, 4)
    plane = [lax.rem(y + dy, 4) * 4 + lax.rem(z + dz, 4) for dy, dz in PLANE]
    line = [lax.rem(x + dx, 4) * 2 + lax.rem(c + dc, 2) for dx, dc in LINE]
    xs = [lax.rem(x + d, 4) for d in (1, 3, 2)]
    ys = [lax.rem(y + d, 4) for d in (1, 3, 2)]
    zs = [lax.rem(z + d, 4) for d in (1, 3, 2)]
    other = 1 - c
    partner = {"gx": x * 2 + other}

    def push(name, h, src, dst, where):
        pltpu.make_async_remote_copy(
            src_ref=src, dst_ref=dst, send_sem=send.at[AT[name, h]], recv_sem=recv.at[AT[name, h]], device_id=where, device_id_type=MESH
        ).start()

    def keep(name, h, src, dst):
        pltpu.make_async_copy(src, dst, recv.at[AT[name, h]]).start()

    def got(name, h, ref):
        pltpu.make_async_copy(ref, ref, recv.at[AT[name, h]]).wait()

    def sent(name, h, ref):
        pltpu.make_async_copy(ref, ref, send.at[AT[name, h]]).wait()

    def cols(g):
        return pl.ds(pl.multiple_of(g * 1024, 1024), 1024)

    def lanes(g):
        return pl.ds(pl.multiple_of(g * 128, 128), 128)

    def rows(m, n):
        return pl.ds(pl.multiple_of(m * n, n), n)

    def s1u_(h):
        for p in plane:
            push("s1u", h, up.at[h, p], s1u.at[h, gy], {"gy": p})
        keep("s1u", h, up.at[h, gy], s1u.at[h, gy])

    def s1d_(h):
        for p in line:
            push("s1d", h, down.at[h, :, :, cols(p)], s1d.at[h, gx], {"gx": p})
        keep("s1d", h, down.at[h, :, :, cols(gx)], s1d.at[h, gx])

    def s2u_(h):
        got("s1u", h, s1u.at[h])
        for p in line:
            push("s2u", h, s1u.at[h, :, :, cols(p)], s2u.at[h, gx], {"gx": p})
        keep("s2u", h, s1u.at[h, :, :, cols(gx)], s2u.at[h, gx])

    def s2d_(h):
        got("s1d", h, s1d.at[h])
        for p in plane:
            push("s2d", h, s1d.at[h, :, p], s2d.at[h, :, gy], {"gy": p})
        keep("s2d", h, s1d.at[h, :, gy], s2d.at[h, :, gy])

    def permute(spread, picked, h):
        def one(m, carry):
            s = source[m * 2 + h]
            picked[h, m // 16, lax.rem(m, 16)] = spread[lax.rem(s, 2), s // 32, lax.rem(s // 2, 16)]
            return carry

        lax.fori_loop(0, 128, one, 0, unroll=4)

    def s3u_(h):
        for p in line:
            push("s3u", h, pu.at[h, p], s3u.at[h, :, :, cols(gx)], {"gx": p})
        keep("s3u", h, pu.at[h, gx], s3u.at[h, :, :, cols(gx)])

    def s3d_(h):
        for p in plane:
            push("s3d", h, pd.at[h, :, p], s3d.at[h, :, gy], {"gy": p})
        keep("s3d", h, pd.at[h, :, gy], s3d.at[h, :, gy])

    def s4u_(h):
        got("s3u", h, s3u.at[h])
        for p in plane:
            push("s4u", h, s3u.at[h, p], up_new.at[h, gy], {"gy": p})
        keep("s4u", h, s3u.at[h, gy], up_new.at[h, gy])

    def s4d_(h):
        got("s3d", h, s3d.at[h])
        for p in line:
            push("s4d", h, s3d.at[h, p], down_new.at[h, :, :, cols(gx)], {"gx": p})
        keep("s4d", h, s3d.at[h, gx], down_new.at[h, :, :, cols(gx)])

    def reorder_tokens():
        def some(m, carry):
            at_rows = rows(m, 128)
            pick = jnp.where(route[at_rows, :] == lax.broadcasted_iota(jnp.int32, (128, 512), 1), 1.0, 0.0).astype(BF)
            for n in range(2):
                part = t[:, :, :, pl.ds(n * 512, 512)].reshape(512, 512)
                to[at_rows, pl.ds(n * 512, 512)] = jnp.dot(pick, part, preferred_element_type=F32).astype(BF)
            return carry

        lax.fori_loop(0, 4, some, 0)

    def first_product(h):
        def some(q, carry):
            w = s2u[h, pl.ds(q * 2, 2)].astype(F32).reshape(256, 1024).astype(BF)
            for m in range(2):
                a = to[pl.ds(m * 256, 256), :]
                pr[h, q, pl.ds(m * 256, 256), :] = lax.dot_general(a, w, (((1,), (1,)), ((), ())), preferred_element_type=F32)
            return carry

        lax.fori_loop(0, 4, some, 0)
        push("pc", h, pr.at[h, :, :, lanes(other)], pc.at[h], partner)

    def over_cores(h):
        got("pc", h, pc.at[h])

        def some(m, carry):
            q, at_rows = m // 4, rows(lax.rem(m, 4), 128)
            pc[h, q, at_rows, :] = pc[h, q, at_rows, :] + pr[h, q, at_rows, lanes(c)]
            return carry

        lax.fori_loop(0, 16, some, 0)
        for i, p in enumerate(xs):
            push("px", h, pc.at[h, p], px.at[h, i], {"gx": p * 2 + c})

    def activate():
        for h in (0, 1):
            got("px", h, px.at[h])

            def some(m, carry):
                at_rows = rows(m, 128)
                total = pc[h, x, at_rows, :] + px[h, 0, at_rows, :] + px[h, 1, at_rows, :] + px[h, 2, at_rows, :]
                hb[gx, at_rows, pl.ds(h * 128, 128)] = gelu(total).astype(BF)
                return carry

            lax.fori_loop(0, 4, some, 0)
        for p in xs:
            push("hx", 0, hb.at[gx], hb.at[gx], {"gx": p * 2 + c})
        push("hc", 0, hb.at[gx], hb.at[gx], partner)

    def share_hidden():
        got("hx", 0, hb.at[pl.ds(0, 3)])
        for p in xs:
            push("hd", 0, hb.at[p * 2 + c], hb.at[p * 2 + c], partner)

    def second_product():
        got("hc", 0, hb.at[0])
        got("hd", 0, hb.at[pl.ds(0, 3)])
        acc[...] = jnp.zeros_like(acc)

        def some(q, carry):
            w = s2d[:, q].astype(F32).reshape(256, 1024).astype(BF)
            for m in range(2):
                for n in range(2):
                    at_rows, at_cols = pl.ds(m * 256, 256), pl.ds(n * 512, 512)
                    part = jnp.dot(hb[q, at_rows, :], w[:, n * 512 : n * 512 + 512], preferred_element_type=F32)
                    acc[at_rows, at_cols] += part
            return carry

        lax.fori_loop(0, 8, some, 0)

        def rounded(m, carry):
            at_rows = rows(m, 32)
            sc[at_rows, :] = acc[at_rows, :].astype(BF)
            return carry

        lax.fori_loop(0, 16, rounded, 0)
        for i, p in enumerate(ys):
            push("ry", 0, sc.at[rows(p, 128), :], ry.at[i], {"gy": p * 4 + z})

    def over_y():
        got("ry", 0, ry)

        def some(m, carry):
            at_rows = pl.ds(pl.multiple_of(y * 128 + m * 32, 32), 32)
            total = acc[at_rows, :]
            for i in range(3):
                total = total + ry[i, rows(m, 32), :].astype(F32)
            acc[at_rows, :] = total
            sz[rows(m, 32), :] = total.astype(BF)
            return carry

        lax.fori_loop(0, 4, some, 0)
        for i, p in enumerate(zs):
            push("rz", 0, sz.at[rows(p, 32), :], rz.at[i], {"gy": y * 4 + p})

    def over_z():
        got("rz", 0, rz)
        total = acc[pl.ds(pl.multiple_of(y * 128 + z * 32, 32), 32), :]
        for i in range(3):
            total = total + rz[i].astype(F32)
        mixed[...] = total.astype(BF)

    barrier = pltpu.get_barrier_semaphore()
    for p in plane:
        pl.semaphore_signal(barrier, inc=1, device_id={"gy": p}, device_id_type=MESH)
    for p in line:
        pl.semaphore_signal(barrier, inc=1, device_id={"gx": p}, device_id_type=MESH)
    pl.semaphore_wait(barrier, len(PLANE) + len(LINE))

    keep("tok", 0, tokens, t.at[y, z])
    for p in ys:
        push("agy", 0, tokens, t.at[y, z], {"gy": p * 4 + z})
    s1u_(0)
    s1d_(0)
    s1d_(1)
    got("tok", 0, tokens)
    got("agy", 0, t.at[0, pl.ds(0, 3)])
    for p in zs:
        push("agz", 0, t.at[:, z], t.at[:, z], {"gy": y * 4 + p})
    s1u_(1)
    s2u_(0)
    s2d_(0)
    got("agz", 0, t.at[:, pl.ds(0, 3)])
    reorder_tokens()
    s2d_(1)
    s2u_(1)
    got("s2u", 0, s2u.at[0])
    first_product(0)
    over_cores(0)
    got("s2u", 1, s2u.at[1])
    first_product(1)
    permute(s2u, pu, 0)
    over_cores(1)
    s3u_(0)
    got("s2d", 0, s2d.at[0])
    got("s2d", 1, s2d.at[1])
    permute(s2d, pd, 0)
    s3d_(0)
    permute(s2d, pd, 1)
    s3d_(1)
    activate()
    permute(s2u, pu, 1)
    s3u_(1)
    s4u_(0)
    share_hidden()
    second_product()
    s4d_(0)
    over_y()
    s4u_(1)
    s4d_(1)
    over_z()

    for h in (0, 1):
        got("s4u", h, s1u.at[h])
        got("s4d", h, s1d.at[h])
    for h in (0, 1):
        for name in ("s1u", "s2d", "s3d", "s4u"):
            sent(name, h, s1u.at[h, pl.ds(0, 15)])
        for name in ("s1d", "s2u", "s3u", "s4d"):
            sent(name, h, s1d.at[h, pl.ds(0, 7)])
        sent("pc", h, pc.at[h])
        sent("px", h, px.at[h])
    sent("agy", 0, t.at[0, pl.ds(0, 3)])
    sent("agz", 0, t.at[:, pl.ds(0, 3)])
    sent("hx", 0, hb.at[pl.ds(0, 3)])
    sent("hc", 0, hb.at[0])
    sent("hd", 0, hb.at[pl.ds(0, 3)])
    sent("ry", 0, ry)
    sent("rz", 0, rz)


def shards(tokens, up_old, down_old, old_slot, new_owner, hot_rank, route):
    new_slot = new_owner * 2 + hot_rank
    slots = lax.broadcasted_iota(jnp.int32, (256, 256), 0)
    source = jnp.sum(jnp.where(slots == new_slot[None, :], old_slot[None, :], 0), axis=1)
    up4, down4 = up_old.reshape(2, 16, 8, 8192), down_old.reshape(2, 16, 8, 8192)
    any_, vmem = pl.BlockSpec(memory_space=pl.ANY), pl.BlockSpec(memory_space=pltpu.VMEM)
    block = jax.ShapeDtypeStruct((2, 16, 8, 8192), BF)
    tiles = jax.ShapeDtypeStruct((2, 8, 16, 8, 1024), BF)
    outs = pl.pallas_call(
        kernel,
        out_shape=(block, block, jax.ShapeDtypeStruct((32, 1024), BF), block, tiles, block, tiles),
        in_specs=[pl.BlockSpec(memory_space=pltpu.SMEM), vmem, any_, any_, any_],
        out_specs=(any_, any_, vmem, any_, any_, any_, any_),
        scratch_shapes=[
            pltpu.VMEM((2, 8, 16, 8, 1024), BF), pltpu.VMEM((2, 8, 16, 8, 1024), BF),
            pltpu.VMEM((2, 8, 16, 8, 1024), BF), pltpu.VMEM((2, 8, 16, 8, 1024), BF),
            pltpu.VMEM((4, 4, 32, 1024), BF), pltpu.VMEM((512, 1024), BF),
            pltpu.VMEM((2, 4, 512, 256), F32), pltpu.VMEM((2, 4, 512, 128), F32), pltpu.VMEM((2, 3, 512, 128), F32),
            pltpu.VMEM((512, 256), BF), pltpu.VMEM((8, 512, 256), BF),
            pltpu.VMEM((512, 1024), F32), pltpu.VMEM((512, 1024), BF),
            pltpu.VMEM((3, 128, 1024), BF), pltpu.VMEM((128, 1024), BF), pltpu.VMEM((3, 32, 1024), BF),
            pltpu.SemaphoreType.DMA((len(AT),)), pltpu.SemaphoreType.DMA((len(AT),)),
        ],
        compiler_params=pltpu.CompilerParams(collective_id=0, has_side_effects=True, vmem_limit_bytes=67043328),
    )(source, route.reshape(512, 1), tokens, up4, down4)
    return outs[0].reshape(256, 8192), outs[1].reshape(256, 8192), outs[2]


def solution(mesh):
    in_specs = (P("gy", "gx"), P(("gx", "gy"), None), P(("gx", "gy"), None), P(), P(), P(), P())
    out_specs = (P(("gx", "gy"), None), P(("gx", "gy"), None), P("gy", "gx"))
    return jax.shard_map(shards, mesh=mesh, in_specs=in_specs, out_specs=out_specs, check_vma=False)
```

```python
import jax
import jax.numpy as jnp
from jax import lax
from jax.experimental import pallas as pl
from jax.experimental.pallas import tpu as pltpu
from jax.sharding import PartitionSpec as P

MESH = pl.DeviceIdType.MESH
BF = jnp.bfloat16
F32 = jnp.float32

PLANE = ((1, 0), (0, 1), (3, 0), (0, 3), (1, 3), (3, 1), (2, 0), (0, 2), (1, 1), (3, 3), (2, 1), (2, 3), (1, 2), (3, 2), (2, 2))
LINE = ((0, 1), (1, 0), (3, 0), (1, 1), (3, 1), (2, 0), (2, 1))

ERFC_P = (2.326819970068386e-2, -1.387039388740657e-1, 3.687424674597105e-1, -5.824733027278666e-1, 6.210004621745983e-1,
          -4.944515323274145e-1, 3.404879937665872e-1, -2.741127028184656e-1, 5.638259427386472e-1)
ERFC_R = (-1.047766399936249e1, 1.297719955372516e1, -7.495518717768503e0, 2.921019019210786e0, -1.015265279202700e0,
          4.218463358204948e-1, -2.820767439740514e-1, 5.641895067754075e-1)
ERF_T = (7.853861353153693e-5, -8.010193625184903e-4, 5.188327685732524e-3, -2.685381193529856e-2, 1.128358514861418e-1,
         -3.761262582423300e-1, 1.128379165726710e0)


def poly(y, coefficients):
    total = jnp.full_like(y, coefficients[0])
    for c in coefficients[1:]:
        total = total * y + c
    return total


def erfc(v):
    size = jnp.maximum(jnp.abs(v), 0.5)
    q = 1.0 / size
    y = q * q
    tail = jnp.exp(-v * v) * q * jnp.where(size < 2.0, poly(y, ERFC_P), poly(y, ERFC_R))
    far = jnp.where(v < 0.0, 2.0 - tail, tail)
    near = 1.0 - v * poly(v * v, ERF_T)
    return jnp.where(jnp.abs(v) > 1.0, far, near)


def gelu(v):
    return 0.5 * v * erfc(v * -0.7071067811865476)


HALF = (0, 1)
NAMES = ("s1u", "s1d", "s2u", "s2d", "s3u", "s3d", "s4u", "s4d", "pc", "px")
SINGLE = ("tok", "agy", "agz", "hx", "hc", "hd", "ry", "rz")
AT = {(name, h): 2 * i + h for i, name in enumerate(NAMES) for h in (0, 1)}
AT.update({(name, 0): 2 * len(NAMES) + i for i, name in enumerate(SINGLE)})


def kernel(source, route, tokens, up, down, up_new, down_new, mixed, s1u, s1d, s3u, s3d,
           s2u, s2d, pu, pd, t, to, pr, pc, pb, px, hb, acc, sc, ry, sz, rz, send, recv):
    gx, gy = lax.axis_index("gx"), lax.axis_index("gy")
    x, c = gx // 2, lax.rem(gx, 2)
    y, z = gy // 4, lax.rem(gy, 4)
    plane = [lax.rem(y + dy, 4) * 4 + lax.rem(z + dz, 4) for dy, dz in PLANE]
    line = [lax.rem(x + dx, 4) * 2 + lax.rem(c + dc, 2) for dx, dc in LINE]
    xs = [lax.rem(x + d, 4) for d in (1, 3, 2)]
    ys = [lax.rem(y + d, 4) for d in (1, 3, 2)]
    zs = [lax.rem(z + d, 4) for d in (1, 3, 2)]
    other = 1 - c
    partner = {"gx": x * 2 + other}

    def push(name, h, src, dst, where):
        pltpu.make_async_remote_copy(
            src_ref=src, dst_ref=dst, send_sem=send.at[AT[name, h]], recv_sem=recv.at[AT[name, h]], device_id=where, device_id_type=MESH
        ).start()

    def keep(name, h, src, dst):
        pltpu.make_async_copy(src, dst, recv.at[AT[name, h]]).start()

    def got(name, h, ref):
        pltpu.make_async_copy(ref, ref, recv.at[AT[name, h]]).wait()

    def sent(name, h, ref):
        pltpu.make_async_copy(ref, ref, send.at[AT[name, h]]).wait()

    def cols(g):
        return pl.ds(pl.multiple_of(g * 1024, 1024), 1024)

    def wide(k):
        return pl.ds(k * 4096, 4096)

    def four(k):
        return pl.ds(k * 4, 4)

    def lanes(g):
        return pl.ds(pl.multiple_of(g * 128, 128), 128)

    def rows(m, n):
        return pl.ds(pl.multiple_of(m * n, n), n)

    def s1u_(h):
        for k in HALF:
            for p in plane:
                push("s1u", h, up.at[h, p, :, wide(k)], s1u.at[h, gy, :, wide(k)], {"gy": p})
        keep("s1u", h, up.at[h, gy], s1u.at[h, gy])

    def s1d_(h):
        for p in line:
            push("s1d", h, down.at[h, :, :, cols(p)], s1d.at[h, gx], {"gx": p})
        keep("s1d", h, down.at[h, :, :, cols(gx)], s1d.at[h, gx])

    def s2u_(h):
        got("s1u", h, s1u.at[h])
        for p in line:
            push("s2u", h, s1u.at[h, :, :, cols(p)], s2u.at[h, gx], {"gx": p})
        keep("s2u", h, s1u.at[h, :, :, cols(gx)], s2u.at[h, gx])

    def s2d_(h):
        got("s1d", h, s1d.at[h])
        for k in HALF:
            for p in plane:
                push("s2d", h, s1d.at[h, four(k), p], s2d.at[h, four(k), gy], {"gy": p})
        keep("s2d", h, s1d.at[h, :, gy], s2d.at[h, :, gy])

    def pick(spread, picked, h, g, r):
        s = source[(g * 16 + r) * 2 + h]
        picked[h, g, r] = spread[lax.rem(s, 2), s // 32, lax.rem(s // 2, 16)]

    def s3u_(h):
        for p in [*line, gx]:
            def one(r, carry):
                pick(s2u, pu, h, p, r)
                return carry

            lax.fori_loop(0, 16, one, 0, unroll=4)
            if p is gx:
                keep("s3u", h, pu.at[h, p], s3u.at[h, :, :, cols(gx)])
            else:
                push("s3u", h, pu.at[h, p], s3u.at[h, :, :, cols(gx)], {"gx": p})

    def s3d_(h):
        for k in HALF:
            for p in [*plane, gy]:
                def one(g, carry):
                    pick(s2d, pd, h, k * 4 + g, p)
                    return carry

                lax.fori_loop(0, 4, one, 0, unroll=4)
                if p is gy:
                    keep("s3d", h, pd.at[h, four(k), p], s3d.at[h, four(k), gy])
                else:
                    push("s3d", h, pd.at[h, four(k), p], s3d.at[h, four(k), gy], {"gy": p})

    def s4u_(h):
        got("s3u", h, s3u.at[h])
        for k in HALF:
            for p in plane:
                push("s4u", h, s3u.at[h, p, :, wide(k)], up_new.at[h, gy, :, wide(k)], {"gy": p})
        keep("s4u", h, s3u.at[h, gy], up_new.at[h, gy])

    def s4d_(h):
        got("s3d", h, s3d.at[h])
        for p in line:
            push("s4d", h, s3d.at[h, p], down_new.at[h, :, :, cols(gx)], {"gx": p})
        keep("s4d", h, s3d.at[h, gx], down_new.at[h, :, :, cols(gx)])

    def reorder_tokens():
        def some(m, carry):
            at_rows = rows(m, 128)
            pick = jnp.where(route[at_rows, :] == lax.broadcasted_iota(jnp.int32, (128, 512), 1), 1.0, 0.0).astype(BF)
            for n in range(2):
                part = t[:, :, :, pl.ds(n * 512, 512)].reshape(512, 512)
                to[at_rows, pl.ds(n * 512, 512)] = jnp.dot(pick, part, preferred_element_type=F32).astype(BF)
            return carry

        lax.fori_loop(0, 4, some, 0)

    def first_product(h):
        def some(q, carry):
            w = s2u[h, pl.ds(q * 2, 2)].astype(F32).reshape(256, 1024).astype(BF)
            for m in range(2):
                a = to[pl.ds(m * 256, 256), :]
                pr[h, q, pl.ds(m * 256, 256), :] = lax.dot_general(a, w, (((1,), (1,)), ((), ())), preferred_element_type=F32)
            return carry

        lax.fori_loop(0, 4, some, 0)
        push("pc", h, pr.at[h, :, :, lanes(other)], pc.at[h], partner)

    def over_cores(h):
        got("pc", h, pc.at[h])

        def some(m, carry):
            q, at_rows = m // 4, rows(lax.rem(m, 4), 128)
            total = pc[h, q, at_rows, :] + pr[h, q, at_rows, lanes(c)]
            pc[h, q, at_rows, :] = total
            pb[h, q, at_rows, :] = total.astype(BF)
            return carry

        lax.fori_loop(0, 16, some, 0)
        for i, p in enumerate(xs):
            push("px", h, pb.at[h, p], px.at[h, i], {"gx": p * 2 + c})

    def activate():
        for h in (0, 1):
            got("px", h, px.at[h])

            def some(m, carry):
                at_rows = rows(m, 128)
                total = pc[h, x, at_rows, :]
                for i in range(3):
                    total = total + px[h, i, at_rows, :].astype(F32)
                hb[gx, at_rows, pl.ds(h * 128, 128)] = gelu(total).astype(BF)
                return carry

            lax.fori_loop(0, 4, some, 0)
        for p in xs:
            push("hx", 0, hb.at[gx], hb.at[gx], {"gx": p * 2 + c})
        push("hc", 0, hb.at[gx], hb.at[gx], partner)

    def share_hidden():
        got("hx", 0, hb.at[pl.ds(0, 3)])
        for p in xs:
            push("hd", 0, hb.at[p * 2 + c], hb.at[p * 2 + c], partner)

    def second_product():
        got("hc", 0, hb.at[0])
        got("hd", 0, hb.at[pl.ds(0, 3)])
        acc[...] = jnp.zeros_like(acc)

        def some(q, carry):
            w = s2d[:, q].astype(F32).reshape(256, 1024).astype(BF)
            for m in range(2):
                for n in range(2):
                    at_rows, at_cols = pl.ds(m * 256, 256), pl.ds(n * 512, 512)
                    part = jnp.dot(hb[q, at_rows, :], w[:, n * 512 : n * 512 + 512], preferred_element_type=F32)
                    acc[at_rows, at_cols] += part
            return carry

        lax.fori_loop(0, 8, some, 0)

        def rounded(m, carry):
            at_rows = rows(m, 32)
            sc[at_rows, :] = acc[at_rows, :].astype(BF)
            return carry

        lax.fori_loop(0, 16, rounded, 0)
        for i, p in enumerate(ys):
            push("ry", 0, sc.at[rows(p, 128), :], ry.at[i], {"gy": p * 4 + z})

    def over_y():
        got("ry", 0, ry)

        def some(m, carry):
            at_rows = pl.ds(pl.multiple_of(y * 128 + m * 32, 32), 32)
            total = acc[at_rows, :]
            for i in range(3):
                total = total + ry[i, rows(m, 32), :].astype(F32)
            acc[at_rows, :] = total
            sz[rows(m, 32), :] = total.astype(BF)
            return carry

        lax.fori_loop(0, 4, some, 0)
        for i, p in enumerate(zs):
            push("rz", 0, sz.at[rows(p, 32), :], rz.at[i], {"gy": y * 4 + p})

    def over_z():
        got("rz", 0, rz)
        total = acc[pl.ds(pl.multiple_of(y * 128 + z * 32, 32), 32), :]
        for i in range(3):
            total = total + rz[i].astype(F32)
        mixed[...] = total.astype(BF)

    barrier = pltpu.get_barrier_semaphore()
    for p in plane:
        pl.semaphore_signal(barrier, inc=1, device_id={"gy": p}, device_id_type=MESH)
    for p in line:
        pl.semaphore_signal(barrier, inc=1, device_id={"gx": p}, device_id_type=MESH)
    pl.semaphore_wait(barrier, len(PLANE) + len(LINE))

    keep("tok", 0, tokens, t.at[y, z])
    for p in ys:
        push("agy", 0, tokens, t.at[y, z], {"gy": p * 4 + z})
    s1u_(0)
    s1d_(0)
    s1d_(1)
    got("tok", 0, tokens)
    got("agy", 0, t.at[0, pl.ds(0, 3)])
    for p in zs:
        push("agz", 0, t.at[:, z], t.at[:, z], {"gy": y * 4 + p})
    s1u_(1)
    s2u_(0)
    s2d_(0)
    got("agz", 0, t.at[:, pl.ds(0, 3)])
    reorder_tokens()
    s2d_(1)
    s2u_(1)
    got("s2u", 0, s2u.at[0])
    first_product(0)
    over_cores(0)
    got("s2u", 1, s2u.at[1])
    first_product(1)
    over_cores(1)
    s3u_(0)
    got("s2d", 0, s2d.at[0])
    got("s2d", 1, s2d.at[1])
    s3d_(0)
    s3d_(1)
    activate()
    s3u_(1)
    s4u_(0)
    share_hidden()
    second_product()
    s4d_(0)
    over_y()
    s4u_(1)
    s4d_(1)
    over_z()

    for h in (0, 1):
        got("s4u", h, s1u.at[h])
        got("s4d", h, s1d.at[h])
    for h in (0, 1):
        for name in ("s1u", "s2d", "s3d", "s4u"):
            sent(name, h, s1u.at[h, pl.ds(0, 15)])
        for name in ("s1d", "s2u", "s3u", "s4d"):
            sent(name, h, s1d.at[h, pl.ds(0, 7)])
        sent("pc", h, pc.at[h])
        sent("px", h, px.at[h])
    sent("agy", 0, t.at[0, pl.ds(0, 3)])
    sent("agz", 0, t.at[:, pl.ds(0, 3)])
    sent("hx", 0, hb.at[pl.ds(0, 3)])
    sent("hc", 0, hb.at[0])
    sent("hd", 0, hb.at[pl.ds(0, 3)])
    sent("ry", 0, ry)
    sent("rz", 0, rz)


def shards(tokens, up_old, down_old, old_slot, new_owner, hot_rank, route):
    new_slot = new_owner * 2 + hot_rank
    slots = lax.broadcasted_iota(jnp.int32, (256, 256), 0)
    source = jnp.sum(jnp.where(slots == new_slot[None, :], old_slot[None, :], 0), axis=1)
    up4, down4 = up_old.reshape(2, 16, 8, 8192), down_old.reshape(2, 16, 8, 8192)
    any_, vmem = pl.BlockSpec(memory_space=pl.ANY), pl.BlockSpec(memory_space=pltpu.VMEM)
    block = jax.ShapeDtypeStruct((2, 16, 8, 8192), BF)
    tiles = jax.ShapeDtypeStruct((2, 8, 16, 8, 1024), BF)
    outs = pl.pallas_call(
        kernel,
        out_shape=(block, block, jax.ShapeDtypeStruct((32, 1024), BF), block, tiles, block, tiles),
        in_specs=[pl.BlockSpec(memory_space=pltpu.SMEM), vmem, any_, any_, any_],
        out_specs=(any_, any_, vmem, any_, any_, any_, any_),
        scratch_shapes=[
            pltpu.VMEM((2, 8, 16, 8, 1024), BF), pltpu.VMEM((2, 8, 16, 8, 1024), BF),
            pltpu.VMEM((2, 8, 16, 8, 1024), BF), pltpu.VMEM((2, 8, 16, 8, 1024), BF),
            pltpu.VMEM((4, 4, 32, 1024), BF), pltpu.VMEM((512, 1024), BF),
            pltpu.VMEM((2, 4, 512, 256), F32), pltpu.VMEM((2, 4, 512, 128), F32), pltpu.VMEM((2, 4, 512, 128), BF), pltpu.VMEM((2, 3, 512, 128), BF),
            pltpu.VMEM((8, 512, 256), BF),
            pltpu.VMEM((512, 1024), F32), pltpu.VMEM((512, 1024), BF),
            pltpu.VMEM((3, 128, 1024), BF), pltpu.VMEM((128, 1024), BF), pltpu.VMEM((3, 32, 1024), BF),
            pltpu.SemaphoreType.DMA((len(AT),)), pltpu.SemaphoreType.DMA((len(AT),)),
        ],
        compiler_params=pltpu.CompilerParams(collective_id=0, has_side_effects=True, vmem_limit_bytes=67043328),
    )(source, route.reshape(512, 1), tokens, up4, down4)
    return outs[0].reshape(256, 8192), outs[1].reshape(256, 8192), outs[2]


def solution(mesh):
    in_specs = (P("gy", "gx"), P(("gx", "gy"), None), P(("gx", "gy"), None), P(), P(), P(), P())
    out_specs = (P(("gx", "gy"), None), P(("gx", "gy"), None), P("gy", "gx"))
    return jax.shard_map(shards, mesh=mesh, in_specs=in_specs, out_specs=out_specs, check_vma=False)
```

```python
import jax
import jax.numpy as jnp
from jax import lax
from jax.experimental import pallas as pl
from jax.experimental.pallas import tpu as pltpu
from jax.sharding import PartitionSpec as P

MESH = pl.DeviceIdType.MESH
BF = jnp.bfloat16
F32 = jnp.float32

PLANE = ((1, 0), (0, 1), (3, 0), (0, 3), (1, 3), (3, 1), (2, 0), (0, 2), (1, 1), (3, 3), (2, 1), (2, 3), (1, 2), (3, 2), (2, 2))
LINE = ((0, 1), (1, 0), (3, 0), (1, 1), (3, 1), (2, 0), (2, 1))

ERFC_P = (2.326819970068386e-2, -1.387039388740657e-1, 3.687424674597105e-1, -5.824733027278666e-1, 6.210004621745983e-1,
          -4.944515323274145e-1, 3.404879937665872e-1, -2.741127028184656e-1, 5.638259427386472e-1)
ERFC_R = (-1.047766399936249e1, 1.297719955372516e1, -7.495518717768503e0, 2.921019019210786e0, -1.015265279202700e0,
          4.218463358204948e-1, -2.820767439740514e-1, 5.641895067754075e-1)
ERF_T = (7.853861353153693e-5, -8.010193625184903e-4, 5.188327685732524e-3, -2.685381193529856e-2, 1.128358514861418e-1,
         -3.761262582423300e-1, 1.128379165726710e0)


def poly(y, coefficients):
    total = jnp.full_like(y, coefficients[0])
    for c in coefficients[1:]:
        total = total * y + c
    return total


def erfc(v):
    size = jnp.maximum(jnp.abs(v), 0.5)
    q = 1.0 / size
    y = q * q
    tail = jnp.exp(-v * v) * q * jnp.where(size < 2.0, poly(y, ERFC_P), poly(y, ERFC_R))
    far = jnp.where(v < 0.0, 2.0 - tail, tail)
    near = 1.0 - v * poly(v * v, ERF_T)
    return jnp.where(jnp.abs(v) > 1.0, far, near)


def gelu(v):
    return 0.5 * v * erfc(v * -0.7071067811865476)


HALF = (0, 1)
NAMES = ("s1u", "s1d", "s2u", "s2d", "s3u", "s3d", "s4u", "s4d", "pc", "px")
SINGLE = ("tok", "agy", "agz", "hx", "hc", "hd", "ry", "rz")
AT = {(name, h): 2 * i + h for i, name in enumerate(NAMES) for h in (0, 1)}
AT.update({(name, 0): 2 * len(NAMES) + i for i, name in enumerate(SINGLE)})


def kernel(source, route, tokens, up, down, up_new, down_new, mixed, s1u, s1d, s3u, s3d,
           s2u, s2d, pu, pd, t, to, pr, pc, pb, px, hb, acc, sc, ry, sz, rz, send, recv):
    gx, gy = lax.axis_index("gx"), lax.axis_index("gy")
    x, c = gx // 2, lax.rem(gx, 2)
    y, z = gy // 4, lax.rem(gy, 4)
    plane = [lax.rem(y + dy, 4) * 4 + lax.rem(z + dz, 4) for dy, dz in PLANE]
    line = [lax.rem(x + dx, 4) * 2 + lax.rem(c + dc, 2) for dx, dc in LINE]
    xs = [lax.rem(x + d, 4) for d in (1, 3, 2)]
    ys = [lax.rem(y + d, 4) for d in (1, 3, 2)]
    zs = [lax.rem(z + d, 4) for d in (1, 3, 2)]
    other = 1 - c
    partner = {"gx": x * 2 + other}

    def push(name, h, src, dst, where):
        pltpu.make_async_remote_copy(
            src_ref=src, dst_ref=dst, send_sem=send.at[AT[name, h]], recv_sem=recv.at[AT[name, h]], device_id=where, device_id_type=MESH
        ).start()

    def keep(name, h, src, dst):
        pltpu.make_async_copy(src, dst, recv.at[AT[name, h]]).start()

    def got(name, h, ref):
        pltpu.make_async_copy(ref, ref, recv.at[AT[name, h]]).wait()

    def sent(name, h, ref):
        pltpu.make_async_copy(ref, ref, send.at[AT[name, h]]).wait()

    def cols(g):
        return pl.ds(pl.multiple_of(g * 1024, 1024), 1024)

    def wide(k):
        return pl.ds(k * 4096, 4096)

    def eight(k):
        return pl.ds(k * 8, 8)

    def four(k):
        return pl.ds(k * 4, 4)

    def lanes(g):
        return pl.ds(pl.multiple_of(g * 128, 128), 128)

    def rows(m, n):
        return pl.ds(pl.multiple_of(m * n, n), n)

    def s1u_(h):
        for k in HALF:
            for p in plane:
                push("s1u", h, up.at[h, p, :, wide(k)], s1u.at[h, gy, :, wide(k)], {"gy": p})
        keep("s1u", h, up.at[h, gy], s1u.at[h, gy])

    def s1d_(h):
        for k in HALF:
            for p in line:
                push("s1d", h, down.at[h, eight(k), :, cols(p)], s1d.at[h, gx, eight(k)], {"gx": p})
        keep("s1d", h, down.at[h, :, :, cols(gx)], s1d.at[h, gx])

    def s2u_(h):
        got("s1u", h, s1u.at[h])
        for k in HALF:
            for p in line:
                push("s2u", h, s1u.at[h, eight(k), :, cols(p)], s2u.at[h, gx, eight(k)], {"gx": p})
        keep("s2u", h, s1u.at[h, :, :, cols(gx)], s2u.at[h, gx])

    def s2d_(h):
        got("s1d", h, s1d.at[h])
        for k in HALF:
            for p in plane:
                push("s2d", h, s1d.at[h, four(k), p], s2d.at[h, four(k), gy], {"gy": p})
        keep("s2d", h, s1d.at[h, :, gy], s2d.at[h, :, gy])

    def pick(spread, picked, h, g, r):
        s = source[(g * 16 + r) * 2 + h]
        picked[h, g, r] = spread[lax.rem(s, 2), s // 32, lax.rem(s // 2, 16)]

    def s3u_(h):
        for p in [*line, gx]:
            def one(r, carry):
                pick(s2u, pu, h, p, r)
                return carry

            lax.fori_loop(0, 16, one, 0, unroll=4)
            if p is gx:
                keep("s3u", h, pu.at[h, p], s3u.at[h, :, :, cols(gx)])
            else:
                push("s3u", h, pu.at[h, p], s3u.at[h, :, :, cols(gx)], {"gx": p})

    def s3d_(h):
        for k in HALF:
            for p in [*plane, gy]:
                def one(g, carry):
                    pick(s2d, pd, h, k * 4 + g, p)
                    return carry

                lax.fori_loop(0, 4, one, 0, unroll=4)
                if p is gy:
                    keep("s3d", h, pd.at[h, four(k), p], s3d.at[h, four(k), gy])
                else:
                    push("s3d", h, pd.at[h, four(k), p], s3d.at[h, four(k), gy], {"gy": p})

    def s4u_(h):
        got("s3u", h, s3u.at[h])
        for k in HALF:
            for p in plane:
                push("s4u", h, s3u.at[h, p, :, wide(k)], up_new.at[h, gy, :, wide(k)], {"gy": p})
        keep("s4u", h, s3u.at[h, gy], up_new.at[h, gy])

    def s4d_(h):
        got("s3d", h, s3d.at[h])
        for k in HALF:
            for p in line:
                push("s4d", h, s3d.at[h, p, eight(k)], down_new.at[h, eight(k), :, cols(gx)], {"gx": p})
        keep("s4d", h, s3d.at[h, gx], down_new.at[h, :, :, cols(gx)])

    def reorder_tokens():
        def some(m, carry):
            at_rows = rows(m, 128)
            pick = jnp.where(route[:, at_rows] == lax.broadcasted_iota(jnp.int32, (512, 128), 0), 1.0, 0.0).astype(BF)
            for n in range(2):
                part = t[:, :, :, pl.ds(n * 512, 512)].reshape(512, 512)
                to[at_rows, pl.ds(n * 512, 512)] = lax.dot_general(pick, part, (((0,), (0,)), ((), ())), preferred_element_type=F32).astype(BF)
            return carry

        lax.fori_loop(0, 4, some, 0)

    def first_product(h):
        def some(q, carry):
            w = s2u[h, pl.ds(q * 2, 2)].astype(F32).reshape(256, 1024).astype(BF)
            for m in range(2):
                a = to[pl.ds(m * 256, 256), :]
                pr[h, q, pl.ds(m * 256, 256), :] = lax.dot_general(a, w, (((1,), (1,)), ((), ())), preferred_element_type=F32)
            return carry

        lax.fori_loop(0, 4, some, 0)
        push("pc", h, pr.at[h, :, :, lanes(other)], pc.at[h], partner)

    def over_cores(h):
        got("pc", h, pc.at[h])

        def some(m, carry):
            q, at_rows = m // 4, rows(lax.rem(m, 4), 128)
            total = pc[h, q, at_rows, :] + pr[h, q, at_rows, lanes(c)]
            pc[h, q, at_rows, :] = total
            pb[h, q, at_rows, :] = total.astype(BF)
            return carry

        lax.fori_loop(0, 16, some, 0)
        for i, p in enumerate(xs):
            push("px", h, pb.at[h, p], px.at[h, i], {"gx": p * 2 + c})

    def activate():
        for h in (0, 1):
            got("px", h, px.at[h])

            def some(m, carry):
                at_rows = rows(m, 128)
                total = pc[h, x, at_rows, :]
                for i in range(3):
                    total = total + px[h, i, at_rows, :].astype(F32)
                hb[gx, at_rows, pl.ds(h * 128, 128)] = gelu(total).astype(BF)
                return carry

            lax.fori_loop(0, 4, some, 0)
        for p in xs:
            push("hx", 0, hb.at[gx], hb.at[gx], {"gx": p * 2 + c})
        push("hc", 0, hb.at[gx], hb.at[gx], partner)

    def share_hidden():
        got("hx", 0, hb.at[pl.ds(0, 3)])
        for p in xs:
            push("hd", 0, hb.at[p * 2 + c], hb.at[p * 2 + c], partner)

    def second_product():
        got("hc", 0, hb.at[0])
        got("hd", 0, hb.at[pl.ds(0, 3)])
        acc[...] = jnp.zeros_like(acc)

        def some(q, carry):
            w = s2d[:, q].astype(F32).reshape(256, 1024).astype(BF)
            for m in range(2):
                for n in range(2):
                    at_rows, at_cols = pl.ds(m * 256, 256), pl.ds(n * 512, 512)
                    part = jnp.dot(hb[q, at_rows, :], w[:, n * 512 : n * 512 + 512], preferred_element_type=F32)
                    acc[at_rows, at_cols] += part
            return carry

        lax.fori_loop(0, 8, some, 0)

        def rounded(m, carry):
            at_rows = rows(m, 32)
            sc[at_rows, :] = acc[at_rows, :].astype(BF)
            return carry

        lax.fori_loop(0, 16, rounded, 0)
        for i, p in enumerate(ys):
            push("ry", 0, sc.at[rows(p, 128), :], ry.at[i], {"gy": p * 4 + z})

    def over_y():
        got("ry", 0, ry)

        def some(m, carry):
            at_rows = pl.ds(pl.multiple_of(y * 128 + m * 32, 32), 32)
            total = acc[at_rows, :]
            for i in range(3):
                total = total + ry[i, rows(m, 32), :].astype(F32)
            acc[at_rows, :] = total
            sz[rows(m, 32), :] = total
            return carry

        lax.fori_loop(0, 4, some, 0)
        for i, p in enumerate(zs):
            push("rz", 0, sz.at[rows(p, 32), :], rz.at[i], {"gy": y * 4 + p})

    def over_z():
        got("rz", 0, rz)
        total = acc[pl.ds(pl.multiple_of(y * 128 + z * 32, 32), 32), :]
        for i in range(3):
            total = total + rz[i]
        mixed[...] = total.astype(BF)

    barrier = pltpu.get_barrier_semaphore()
    for p in plane:
        pl.semaphore_signal(barrier, inc=1, device_id={"gy": p}, device_id_type=MESH)
    for p in line:
        pl.semaphore_signal(barrier, inc=1, device_id={"gx": p}, device_id_type=MESH)
    pl.semaphore_wait(barrier, len(PLANE) + len(LINE))

    keep("tok", 0, tokens, t.at[y, z])
    for p in ys:
        push("agy", 0, tokens, t.at[y, z], {"gy": p * 4 + z})
    s1u_(0)
    s1d_(0)
    s1d_(1)
    got("tok", 0, tokens)
    got("agy", 0, t.at[0, pl.ds(0, 3)])
    for p in zs:
        push("agz", 0, t.at[:, z], t.at[:, z], {"gy": y * 4 + p})
    s1u_(1)
    s2u_(0)
    s2d_(0)
    got("agz", 0, t.at[:, pl.ds(0, 3)])
    reorder_tokens()
    s2d_(1)
    s2u_(1)
    got("s2u", 0, s2u.at[0])
    first_product(0)
    over_cores(0)
    got("s2u", 1, s2u.at[1])
    first_product(1)
    over_cores(1)
    s3u_(0)
    got("s2d", 0, s2d.at[0])
    got("s2d", 1, s2d.at[1])
    s3d_(0)
    s3d_(1)
    activate()
    s3u_(1)
    s4u_(0)
    share_hidden()
    second_product()
    s4d_(0)
    s4u_(1)
    s4d_(1)
    over_y()
    over_z()

    for h in (0, 1):
        got("s4u", h, s1u.at[h])
        got("s4d", h, s1d.at[h])
    for h in (0, 1):
        for name in ("s1u", "s2d", "s3d", "s4u"):
            sent(name, h, s1u.at[h, pl.ds(0, 15)])
        for name in ("s1d", "s2u", "s3u", "s4d"):
            sent(name, h, s1d.at[h, pl.ds(0, 7)])
        sent("pc", h, pc.at[h])
        sent("px", h, px.at[h])
    sent("agy", 0, t.at[0, pl.ds(0, 3)])
    sent("agz", 0, t.at[:, pl.ds(0, 3)])
    sent("hx", 0, hb.at[pl.ds(0, 3)])
    sent("hc", 0, hb.at[0])
    sent("hd", 0, hb.at[pl.ds(0, 3)])
    sent("ry", 0, ry)
    sent("rz", 0, rz)


def shards(tokens, up_old, down_old, old_slot, new_owner, hot_rank, route):
    slots = lax.broadcasted_iota(jnp.int32, (256, 256), 0)
    here = (slots // 2 == new_owner[None, :]) & (slots % 2 == hot_rank[None, :])
    source = jnp.sum(jnp.where(here, old_slot[None, :], 0), axis=1)
    up4, down4 = up_old.reshape(2, 16, 8, 8192), down_old.reshape(2, 16, 8, 8192)
    any_, vmem = pl.BlockSpec(memory_space=pl.ANY), pl.BlockSpec(memory_space=pltpu.VMEM)
    block = jax.ShapeDtypeStruct((2, 16, 8, 8192), BF)
    tiles = jax.ShapeDtypeStruct((2, 8, 16, 8, 1024), BF)
    outs = pl.pallas_call(
        kernel,
        out_shape=(block, block, jax.ShapeDtypeStruct((32, 1024), BF), block, tiles, block, tiles),
        in_specs=[pl.BlockSpec(memory_space=pltpu.SMEM), vmem, any_, any_, any_],
        out_specs=(any_, any_, vmem, any_, any_, any_, any_),
        scratch_shapes=[
            pltpu.VMEM((2, 8, 16, 8, 1024), BF), pltpu.VMEM((2, 8, 16, 8, 1024), BF),
            pltpu.VMEM((2, 8, 16, 8, 1024), BF), pltpu.VMEM((2, 8, 16, 8, 1024), BF),
            pltpu.VMEM((4, 4, 32, 1024), BF), pltpu.VMEM((512, 1024), BF),
            pltpu.VMEM((2, 4, 512, 256), F32), pltpu.VMEM((2, 4, 512, 128), F32), pltpu.VMEM((2, 4, 512, 128), BF), pltpu.VMEM((2, 3, 512, 128), BF),
            pltpu.VMEM((8, 512, 256), BF),
            pltpu.VMEM((512, 1024), F32), pltpu.VMEM((512, 1024), BF),
            pltpu.VMEM((3, 128, 1024), BF), pltpu.VMEM((128, 1024), F32), pltpu.VMEM((3, 32, 1024), F32),
            pltpu.SemaphoreType.DMA((len(AT),)), pltpu.SemaphoreType.DMA((len(AT),)),
        ],
        compiler_params=pltpu.CompilerParams(collective_id=0, has_side_effects=True, vmem_limit_bytes=67043328),
    )(source, route.reshape(1, 512), tokens, up4, down4)
    return outs[0].reshape(256, 8192), outs[1].reshape(256, 8192), outs[2]


def solution(mesh):
    in_specs = (P("gy", "gx"), P(("gx", "gy"), None), P(("gx", "gy"), None), P(), P(), P(), P())
    out_specs = (P(("gx", "gy"), None), P(("gx", "gy"), None), P("gy", "gx"))
    return jax.shard_map(shards, mesh=mesh, in_specs=in_specs, out_specs=out_specs, check_vma=False)
```

```python
import jax
import jax.numpy as jnp
from jax import lax
from jax.experimental import pallas as pl
from jax.experimental.pallas import tpu as pltpu
from jax.sharding import PartitionSpec as P

MESH = pl.DeviceIdType.MESH
BF = jnp.bfloat16
F32 = jnp.float32

PLANE = ((1, 0), (0, 1), (3, 0), (0, 3), (1, 3), (3, 1), (2, 0), (0, 2), (1, 1), (3, 3), (2, 1), (2, 3), (1, 2), (3, 2), (2, 2))
LINE = ((0, 1), (1, 0), (3, 0), (1, 1), (3, 1), (2, 0), (2, 1))

ERFC_P = (2.326819970068386e-2, -1.387039388740657e-1, 3.687424674597105e-1, -5.824733027278666e-1, 6.210004621745983e-1,
          -4.944515323274145e-1, 3.404879937665872e-1, -2.741127028184656e-1, 5.638259427386472e-1)
ERFC_R = (-1.047766399936249e1, 1.297719955372516e1, -7.495518717768503e0, 2.921019019210786e0, -1.015265279202700e0,
          4.218463358204948e-1, -2.820767439740514e-1, 5.641895067754075e-1)
ERF_T = (7.853861353153693e-5, -8.010193625184903e-4, 5.188327685732524e-3, -2.685381193529856e-2, 1.128358514861418e-1,
         -3.761262582423300e-1, 1.128379165726710e0)


def poly(y, coefficients):
    total = jnp.full_like(y, coefficients[0])
    for c in coefficients[1:]:
        total = total * y + c
    return total


def erfc(v):
    size = jnp.maximum(jnp.abs(v), 0.5)
    q = 1.0 / size
    y = q * q
    tail = jnp.exp(-v * v) * q * jnp.where(size < 2.0, poly(y, ERFC_P), poly(y, ERFC_R))
    far = jnp.where(v < 0.0, 2.0 - tail, tail)
    near = 1.0 - v * poly(v * v, ERF_T)
    return jnp.where(jnp.abs(v) > 1.0, far, near)


def gelu(v):
    return 0.5 * v * erfc(v * -0.7071067811865476)


HALF = (0, 1)
NAMES = ("s1u", "s1d", "s2u", "s2d", "s3u", "s3d", "s4u", "s4d", "pc", "px")
SINGLE = ("tok", "agy", "agz", "hx", "hc", "hd", "ry", "rz")
AT = {(name, h): 2 * i + h for i, name in enumerate(NAMES) for h in (0, 1)}
AT.update({(name, 0): 2 * len(NAMES) + i for i, name in enumerate(SINGLE)})


def kernel(source, route, tokens, up, down, up_new, down_new, mixed, s1u, s1d, s3u, s3d,
           s2u, s2d, pu, pd, t, to, pr, pc, pb, px, hb, acc, sc, ry, sz, rz, send, recv):
    gx, gy = lax.axis_index("gx"), lax.axis_index("gy")
    x, c = gx // 2, lax.rem(gx, 2)
    y, z = gy // 4, lax.rem(gy, 4)
    plane = [lax.rem(y + dy, 4) * 4 + lax.rem(z + dz, 4) for dy, dz in PLANE]
    line = [lax.rem(x + dx, 4) * 2 + lax.rem(c + dc, 2) for dx, dc in LINE]
    xs = [lax.rem(x + d, 4) for d in (1, 3, 2)]
    ys = [lax.rem(y + d, 4) for d in (1, 3, 2)]
    zs = [lax.rem(z + d, 4) for d in (1, 3, 2)]
    other = 1 - c
    partner = {"gx": x * 2 + other}

    def push(name, h, src, dst, where):
        pltpu.make_async_remote_copy(
            src_ref=src, dst_ref=dst, send_sem=send.at[AT[name, h]], recv_sem=recv.at[AT[name, h]], device_id=where, device_id_type=MESH
        ).start()

    def keep(name, h, src, dst):
        pltpu.make_async_copy(src, dst, recv.at[AT[name, h]]).start()

    def got(name, h, ref):
        pltpu.make_async_copy(ref, ref, recv.at[AT[name, h]]).wait()

    def sent(name, h, ref):
        pltpu.make_async_copy(ref, ref, send.at[AT[name, h]]).wait()

    def cols(g):
        return pl.ds(pl.multiple_of(g * 1024, 1024), 1024)

    def wide(k):
        return pl.ds(k * 4096, 4096)

    def eight(k):
        return pl.ds(k * 8, 8)

    def four(k):
        return pl.ds(k * 4, 4)

    def lanes(g):
        return pl.ds(pl.multiple_of(g * 128, 128), 128)

    def rows(m, n):
        return pl.ds(pl.multiple_of(m * n, n), n)

    def s1u_(h):
        for k in HALF:
            for p in plane:
                push("s1u", h, up.at[h, p, :, wide(k)], s1u.at[h, gy, :, wide(k)], {"gy": p})
        keep("s1u", h, up.at[h, gy], s1u.at[h, gy])

    def s1d_(h):
        for k in HALF:
            for p in line:
                push("s1d", h, down.at[h, eight(k), :, cols(p)], s1d.at[h, gx, eight(k)], {"gx": p})
        keep("s1d", h, down.at[h, :, :, cols(gx)], s1d.at[h, gx])

    def s2u_(h):
        got("s1u", h, s1u.at[h])
        for k in HALF:
            for p in line:
                push("s2u", h, s1u.at[h, eight(k), :, cols(p)], s2u.at[h, gx, eight(k)], {"gx": p})
        keep("s2u", h, s1u.at[h, :, :, cols(gx)], s2u.at[h, gx])

    def s2d_(h):
        got("s1d", h, s1d.at[h])
        for k in HALF:
            for p in plane:
                push("s2d", h, s1d.at[h, four(k), p], s2d.at[h, four(k), gy], {"gy": p})
        keep("s2d", h, s1d.at[h, :, gy], s2d.at[h, :, gy])

    def pick(spread, picked, h, g, r):
        s = source[(g * 16 + r) * 2 + h]
        picked[h, g, r] = spread[lax.rem(s, 2), s // 32, lax.rem(s // 2, 16)]

    def s3u_(h):
        for k in HALF:
            for p in [*line, gx]:
                def one(r, carry):
                    pick(s2u, pu, h, p, k * 8 + r)
                    return carry

                lax.fori_loop(0, 8, one, 0, unroll=4)
                if p is gx:
                    keep("s3u", h, pu.at[h, p, eight(k)], s3u.at[h, eight(k), :, cols(gx)])
                else:
                    push("s3u", h, pu.at[h, p, eight(k)], s3u.at[h, eight(k), :, cols(gx)], {"gx": p})

    def s3d_(h):
        for k in HALF:
            for p in [*plane, gy]:
                def one(g, carry):
                    pick(s2d, pd, h, k * 4 + g, p)
                    return carry

                lax.fori_loop(0, 4, one, 0, unroll=4)
                if p is gy:
                    keep("s3d", h, pd.at[h, four(k), p], s3d.at[h, four(k), gy])
                else:
                    push("s3d", h, pd.at[h, four(k), p], s3d.at[h, four(k), gy], {"gy": p})

    def s4u_(h):
        got("s3u", h, s3u.at[h])
        for k in HALF:
            for p in plane:
                push("s4u", h, s3u.at[h, p, :, wide(k)], up_new.at[h, gy, :, wide(k)], {"gy": p})
        keep("s4u", h, s3u.at[h, gy], up_new.at[h, gy])

    def s4d_(h):
        got("s3d", h, s3d.at[h])
        for k in HALF:
            for p in line:
                push("s4d", h, s3d.at[h, p, eight(k)], down_new.at[h, eight(k), :, cols(gx)], {"gx": p})
        keep("s4d", h, s3d.at[h, gx], down_new.at[h, :, :, cols(gx)])

    def reorder_tokens():
        def some(m, carry):
            at_rows = rows(m, 128)
            pick = jnp.where(route[:, at_rows] == lax.broadcasted_iota(jnp.int32, (512, 128), 0), 1.0, 0.0).astype(BF)
            for n in range(2):
                part = t[:, :, :, pl.ds(n * 512, 512)].reshape(512, 512)
                to[at_rows, pl.ds(n * 512, 512)] = lax.dot_general(pick, part, (((0,), (0,)), ((), ())), preferred_element_type=F32).astype(BF)
            return carry

        lax.fori_loop(0, 4, some, 0)

    def first_product(h):
        def some(q, carry):
            w = s2u[h, pl.ds(q * 2, 2)].astype(F32).reshape(256, 1024).astype(BF)
            for m in range(2):
                a = to[pl.ds(m * 256, 256), :]
                pr[h, q, pl.ds(m * 256, 256), :] = lax.dot_general(a, w, (((1,), (1,)), ((), ())), preferred_element_type=F32)
            return carry

        lax.fori_loop(0, 4, some, 0)
        push("pc", h, pr.at[h, :, :, lanes(other)], pc.at[h], partner)

    def over_cores(h):
        got("pc", h, pc.at[h])

        def some(m, carry):
            q, at_rows = m // 4, rows(lax.rem(m, 4), 128)
            total = pc[h, q, at_rows, :] + pr[h, q, at_rows, lanes(c)]
            pc[h, q, at_rows, :] = total
            pb[h, q, at_rows, :] = total.astype(BF)
            return carry

        lax.fori_loop(0, 16, some, 0)
        for i, p in enumerate(xs):
            push("px", h, pb.at[h, p], px.at[h, i], {"gx": p * 2 + c})

    def activate():
        for h in (0, 1):
            got("px", h, px.at[h])

            def some(m, carry):
                at_rows = rows(m, 128)
                total = pc[h, x, at_rows, :]
                for i in range(3):
                    total = total + px[h, i, at_rows, :].astype(F32)
                hb[gx, at_rows, pl.ds(h * 128, 128)] = gelu(total).astype(BF)
                return carry

            lax.fori_loop(0, 4, some, 0)
        for p in xs:
            push("hx", 0, hb.at[gx], hb.at[gx], {"gx": p * 2 + c})
        push("hc", 0, hb.at[gx], hb.at[gx], partner)

    def share_hidden():
        got("hx", 0, hb.at[pl.ds(0, 3)])
        for p in xs:
            push("hd", 0, hb.at[p * 2 + c], hb.at[p * 2 + c], partner)

    def second_product():
        got("hc", 0, hb.at[0])
        got("hd", 0, hb.at[pl.ds(0, 3)])
        acc[...] = jnp.zeros_like(acc)

        def some(q, carry):
            w = s2d[:, q].astype(F32).reshape(256, 1024).astype(BF)
            for m in range(2):
                for n in range(2):
                    at_rows, at_cols = pl.ds(m * 256, 256), pl.ds(n * 512, 512)
                    part = jnp.dot(hb[q, at_rows, :], w[:, n * 512 : n * 512 + 512], preferred_element_type=F32)
                    acc[at_rows, at_cols] += part
            return carry

        lax.fori_loop(0, 8, some, 0)

        def rounded(m, carry):
            at_rows = rows(m, 32)
            sc[at_rows, :] = acc[at_rows, :].astype(BF)
            return carry

        lax.fori_loop(0, 16, rounded, 0)
        for i, p in enumerate(ys):
            push("ry", 0, sc.at[rows(p, 128), :], ry.at[i], {"gy": p * 4 + z})

    def over_y():
        got("ry", 0, ry)

        def some(m, carry):
            at_rows = pl.ds(pl.multiple_of(y * 128 + m * 32, 32), 32)
            total = acc[at_rows, :]
            for i in range(3):
                total = total + ry[i, rows(m, 32), :].astype(F32)
            acc[at_rows, :] = total
            sz[rows(m, 32), :] = total
            return carry

        lax.fori_loop(0, 4, some, 0)
        for i, p in enumerate(zs):
            push("rz", 0, sz.at[rows(p, 32), :], rz.at[i], {"gy": y * 4 + p})

    def over_z():
        got("rz", 0, rz)
        total = acc[pl.ds(pl.multiple_of(y * 128 + z * 32, 32), 32), :]
        for i in range(3):
            total = total + rz[i]
        mixed[...] = total.astype(BF)

    barrier = pltpu.get_barrier_semaphore()
    for p in plane:
        pl.semaphore_signal(barrier, inc=1, device_id={"gy": p}, device_id_type=MESH)
    for p in line:
        pl.semaphore_signal(barrier, inc=1, device_id={"gx": p}, device_id_type=MESH)
    pl.semaphore_wait(barrier, len(PLANE) + len(LINE))

    keep("tok", 0, tokens, t.at[y, z])
    for p in ys:
        push("agy", 0, tokens, t.at[y, z], {"gy": p * 4 + z})
    s1u_(0)
    s1d_(0)
    s1d_(1)
    got("tok", 0, tokens)
    got("agy", 0, t.at[0, pl.ds(0, 3)])
    for p in zs:
        push("agz", 0, t.at[:, z], t.at[:, z], {"gy": y * 4 + p})
    s1u_(1)
    s2u_(0)
    s2d_(0)
    got("agz", 0, t.at[:, pl.ds(0, 3)])
    reorder_tokens()
    s2d_(1)
    s2u_(1)
    got("s2u", 0, s2u.at[0])
    first_product(0)
    over_cores(0)
    got("s2u", 1, s2u.at[1])
    first_product(1)
    over_cores(1)
    s3u_(0)
    got("s2d", 0, s2d.at[0])
    got("s2d", 1, s2d.at[1])
    s3d_(0)
    s3d_(1)
    activate()
    s3u_(1)
    s4u_(0)
    share_hidden()
    second_product()
    s4d_(0)
    s4u_(1)
    s4d_(1)
    over_y()
    over_z()

    for h in (0, 1):
        got("s4u", h, s1u.at[h])
        got("s4d", h, s1d.at[h])
    for h in (0, 1):
        for name in ("s1u", "s2d", "s3d", "s4u"):
            sent(name, h, s1u.at[h, pl.ds(0, 15)])
        for name in ("s1d", "s2u", "s3u", "s4d"):
            sent(name, h, s1d.at[h, pl.ds(0, 7)])
        sent("pc", h, pc.at[h])
        sent("px", h, px.at[h])
    sent("agy", 0, t.at[0, pl.ds(0, 3)])
    sent("agz", 0, t.at[:, pl.ds(0, 3)])
    sent("hx", 0, hb.at[pl.ds(0, 3)])
    sent("hc", 0, hb.at[0])
    sent("hd", 0, hb.at[pl.ds(0, 3)])
    sent("ry", 0, ry)
    sent("rz", 0, rz)


def shards(tokens, up_old, down_old, old_slot, new_owner, hot_rank, route):
    slots = lax.broadcasted_iota(jnp.int32, (256, 256), 0)
    here = (slots // 2 == new_owner[None, :]) & (slots % 2 == hot_rank[None, :])
    source = jnp.sum(jnp.where(here, old_slot[None, :], 0), axis=1)
    up4, down4 = up_old.reshape(2, 16, 8, 8192), down_old.reshape(2, 16, 8, 8192)
    any_, vmem = pl.BlockSpec(memory_space=pl.ANY), pl.BlockSpec(memory_space=pltpu.VMEM)
    block = jax.ShapeDtypeStruct((2, 16, 8, 8192), BF)
    tiles = jax.ShapeDtypeStruct((2, 8, 16, 8, 1024), BF)
    outs = pl.pallas_call(
        kernel,
        out_shape=(block, block, jax.ShapeDtypeStruct((32, 1024), BF), block, tiles, block, tiles),
        in_specs=[pl.BlockSpec(memory_space=pltpu.SMEM), vmem, any_, any_, any_],
        out_specs=(any_, any_, vmem, any_, any_, any_, any_),
        scratch_shapes=[
            pltpu.VMEM((2, 8, 16, 8, 1024), BF), pltpu.VMEM((2, 8, 16, 8, 1024), BF),
            pltpu.VMEM((2, 8, 16, 8, 1024), BF), pltpu.VMEM((2, 8, 16, 8, 1024), BF),
            pltpu.VMEM((4, 4, 32, 1024), BF), pltpu.VMEM((512, 1024), BF),
            pltpu.VMEM((2, 4, 512, 256), F32), pltpu.VMEM((2, 4, 512, 128), F32), pltpu.VMEM((2, 4, 512, 128), BF), pltpu.VMEM((2, 3, 512, 128), BF),
            pltpu.VMEM((8, 512, 256), BF),
            pltpu.VMEM((512, 1024), F32), pltpu.VMEM((512, 1024), BF),
            pltpu.VMEM((3, 128, 1024), BF), pltpu.VMEM((128, 1024), F32), pltpu.VMEM((3, 32, 1024), F32),
            pltpu.SemaphoreType.DMA((len(AT),)), pltpu.SemaphoreType.DMA((len(AT),)),
        ],
        compiler_params=pltpu.CompilerParams(collective_id=0, has_side_effects=True, vmem_limit_bytes=67043328),
    )(source, route.reshape(1, 512), tokens, up4, down4)
    return outs[0].reshape(256, 8192), outs[1].reshape(256, 8192), outs[2]


def solution(mesh):
    in_specs = (P("gy", "gx"), P(("gx", "gy"), None), P(("gx", "gy"), None), P(), P(), P(), P())
    out_specs = (P(("gx", "gy"), None), P(("gx", "gy"), None), P("gy", "gx"))
    return jax.shard_map(shards, mesh=mesh, in_specs=in_specs, out_specs=out_specs, check_vma=False)
```
